32 devices in a mesh: layer: 4 (over x, core), row: 8 (over z, y).
Axes of the slice: x: 2, y: 2, z: 4, core: 2. Of those that a mesh axis runs over, the one named last changes fastest.
Arguments:
- magnet: float32 [3, 4, 2048, 2048], P(None, 'layer', 'row'), may hold values from -6 to 6
- kernel: float32 [7, 6, 2048, 2048], P(None, None, ('layer', 'row')), may hold values from -1.8 to 1.8, as said below
Outputs:
- demag: float32 [3, 4, 2048, 2048], P(None, 'layer', 'row')
The draws below stay inside these ranges and needn't reach their ends.
Inputs may be any that keep to these rules, and one draw needn't show every extreme that they name: With q' = -q mod 2048 and p' = -p mod 2048: parts 0, 1, 2 satisfy kernel[o, j, q', p] = kernel[o, j, q, p'] = kernel[o, j, q, p]; part 3 changes sign under either mirror; part 4 changes sign under p -> p' and keeps it under q -> q'; part 5 keeps its sign under p -> p' and changes it under q -> q'.
All inputs are finite; a program needn't handle non-finite values.
Results may differ from the reference program's by a relative error of at most 0.0001.
Values sent between devices are 32-bit elements; how exact they have to be, the bound alone decides.
A program may use at most 256 MiB of HBM per device.

```python
import jax
import jax.numpy as jnp

NX = 2048
NY = 2048
PARTS_SIZE = 6
LAYERS = 4
OFFSETS = 7


def mirror_p(values):
    return jnp.roll(jnp.flip(values, -1), 1, -1)


def mirror_q(values):
    return jnp.roll(jnp.flip(values, -2), 1, -2)


def draw_kernel(key, part):
    base = jax.random.normal(jax.random.fold_in(key, 71), (OFFSETS, PARTS_SIZE, NY, NX), jnp.float32) * 0.3
    base = jnp.clip(base, -0.9, 0.9)
    sign_p = jnp.array([1.0, 1.0, 1.0, -1.0, -1.0, 1.0], jnp.float32)[None, :, None, None]
    sign_q = jnp.array([1.0, 1.0, 1.0, -1.0, 1.0, -1.0], jnp.float32)[None, :, None, None]
    flipped_p = mirror_p(base)
    flipped_q = mirror_q(base)
    flipped_both = mirror_q(flipped_p)
    total = base + sign_p * flipped_p + sign_q * flipped_q + sign_p * sign_q * flipped_both
    return (0.5 * total).astype(jnp.float32)


def level_of(own_key, shape, cuts, low, largest):
    loudness, own = 1.0, jax.random.fold_in(own_key, 6)
    for position, parts in cuts:
        heights = jnp.exp(jax.random.uniform(jax.random.fold_in(own, position), (parts,), jnp.float32, low / len(cuts), largest / len(cuts)))
        loudness = loudness * jnp.repeat(heights, shape[position] // parts).reshape([-1 if axis == position else 1 for axis in range(len(shape))])
    return loudness


def bell_draw(own_key, dims, width, bound, pieces=(), kind=jnp.bfloat16):
    values = jax.random.normal(own_key, dims, jnp.float32) * width
    if len(pieces) > 0:
        values = level_of(own_key, dims, pieces, -0.22, 0.18) * values
    return jnp.clip(values, min=-bound, max=bound).astype(kind)


def setup_inputs(seed: int = 0) -> dict:
    key_of = jax.random.split(jax.random.key(seed), 3)
    return {
        "magnet": bell_draw(key_of[0], (3, LAYERS, NX, NY), 1.0, 6.0, ((1, 4), (2, 8)), jnp.float32),
        "kernel": draw_kernel(jax.random.fold_in(key_of[2], 71), 0),
    }


def reference(magnet, kernel):
    layers = magnet.shape[1]
    spectra = jnp.fft.fft2(jnp.swapaxes(magnet, 2, 3))
    results = []
    for target in range(layers):
        field_x = jnp.zeros_like(spectra[0, 0])
        field_y = jnp.zeros_like(spectra[0, 0])
        field_z = jnp.zeros_like(spectra[0, 0])
        for source in range(layers):
            coeffs = kernel[target - source + layers - 1]
            mag_x = spectra[0, source]
            mag_y = spectra[1, source]
            mag_z = spectra[2, source]
            field_x = field_x + coeffs[0] * mag_x + coeffs[3] * mag_y + 1j * coeffs[4] * mag_z
            field_y = field_y + coeffs[3] * mag_x + coeffs[1] * mag_y + 1j * coeffs[5] * mag_z
            field_z = field_z + 1j * coeffs[4] * mag_x + 1j * coeffs[5] * mag_y + coeffs[2] * mag_z
        stacked = jnp.stack([field_x, field_y, field_z])
        results.append(-jnp.real(jnp.fft.ifft2(stacked)))
    demag = jnp.stack(results, axis=1)
    return jnp.swapaxes(demag, 2, 3).astype(jnp.float32)
```

```python
import functools
import math

import jax
import jax.numpy as jnp
import numpy as np
from jax import lax
from jax.experimental import pallas as pl
from jax.experimental.pallas import tpu as pltpu
from jax.sharding import PartitionSpec as P

MESH = pl.DeviceIdType.MESH
SUB, LANE = 8, 128
bf16, f32 = jnp.bfloat16, jnp.float32

high = lax.Precision.HIGH


def phases(left, right, length):
    product = left[:, None] * right[None, :] % length
    theta = product.astype(jnp.float32) * (2.0 * math.pi / length)
    return jnp.cos(theta), jnp.sin(theta)


def product_table(length):
    fine = 32
    idx = jnp.arange(length, dtype=jnp.int32)
    c1, s1 = phases(jnp.arange(length // fine, dtype=jnp.int32) * fine, idx, length)
    c2, s2 = phases(jnp.arange(fine, dtype=jnp.int32), idx, length)
    c1, s1 = c1[:, None], s1[:, None]
    cos = (c1 * c2 - s1 * s2).reshape(length, length)
    sin = (c1 * s2 + s1 * c2).reshape(length, length)
    return cos, sin


def row_table(devices, block, kept, length):
    idx = jnp.arange(length, dtype=jnp.int32)
    c1, s1 = phases(jnp.arange(devices, dtype=jnp.int32) * block, idx, length)
    c2, s2 = phases(jnp.arange(kept, dtype=jnp.int32), idx, length)
    c1, s1 = c1[:, None], s1[:, None]
    pair = jnp.stack([c1 * c2 - s1 * s2, -(c1 * s2 + s1 * c2)], axis=1)
    return pair.reshape(devices * 2 * kept, length)


def general(magnet, kernel):
    n_layer = lax.axis_size("layer")
    n_row = lax.axis_size("row")
    devices = n_row * n_layer
    n_comp, _, x_rows, y_cells = magnet.shape
    block, height = kernel.shape[2], kernel.shape[3]
    kept = block // 2 + 1
    axes = ("layer", "row")

    table = row_table(devices, block, kept, y_cells)
    cos, sin = product_table(height)

    def dot(form, a, b):
        return jnp.einsum(form, a, b, precision=high)

    spec_r, spec_i = [], []
    for c in range(n_comp):
        rows = dot("qy,xy->qx", table, magnet[c, 0])
        moved = lax.all_to_all(
            rows.reshape(devices, 2 * kept, x_rows), axes, split_axis=0, concat_axis=0, tiled=True
        )
        split = moved.reshape(n_layer, n_row, 2, kept, x_rows)
        flat = jnp.transpose(split, (2, 0, 3, 1, 4)).reshape(2 * n_layer * kept, height)
        by_cos = dot("mx,xp->mp", flat, cos).reshape(2, n_layer, kept, height)
        by_sin = dot("mx,xp->mp", flat, sin).reshape(2, n_layer, kept, height)
        spec_r.append(by_cos[0] + by_sin[1])
        spec_i.append(by_cos[1] - by_sin[0])

    row_idx = jnp.arange(kept, dtype=jnp.int32)
    edge = (row_idx == 0) | (row_idx == kept - 1)
    weight = jnp.where(edge, -1.0, -2.0)[:, None] * (1.0 / (height * y_cells))
    coeffs = kernel[:, :, :kept]

    entries = (
        ((0, False), (3, False), (4, True)),
        ((3, False), (1, False), (5, True)),
        ((4, True), (5, True), (2, False)),
    )
    outs = []
    for c in range(n_comp):
        real_rows, imag_rows = [], []
        for target in range(n_layer):
            total_r, total_i = 0.0, 0.0
            for source in range(n_layer):
                offset = target - source + n_layer - 1
                for c2 in range(n_comp):
                    part, turned = entries[c][c2]
                    k = coeffs[offset, part]
                    re, im = spec_r[c2][source], spec_i[c2][source]
                    if turned:
                        total_r = total_r - k * im
                        total_i = total_i + k * re
                    else:
                        total_r = total_r + k * re
                        total_i = total_i + k * im
            real_rows.append(total_r * weight)
            imag_rows.append(total_i * weight)
        field = jnp.stack([jnp.stack(real_rows), jnp.stack(imag_rows)])
        flat = field.reshape(2 * n_layer * kept, height)
        by_cos = dot("mp,px->mx", flat, cos).reshape(2, n_layer, kept, n_row, x_rows)
        by_sin = dot("mp,px->mx", flat, sin).reshape(2, n_layer, kept, n_row, x_rows)
        cells = jnp.stack([by_cos[0] - by_sin[1], by_cos[1] + by_sin[0]], axis=2)
        cells = jnp.transpose(cells, (0, 3, 2, 1, 4)).reshape(devices, 2 * kept, x_rows)
        back = lax.all_to_all(cells, axes, split_axis=0, concat_axis=0, tiled=True)
        outs.append(dot("qx,qy->xy", back.reshape(devices * 2 * kept, x_rows), table))
    return jnp.stack(outs)[:, None]


def wave(angles, length, half):
    product = np.outer(angles, np.arange(half)) % length
    theta = product * (2.0 * np.pi / length)
    return np.stack([np.cos(theta), np.sin(theta)])


def base_tables(block, kept, devices, length):
    half = length // 2
    fine = 32
    coarse = wave(np.arange(half // fine) * fine, length, half)
    small = wave(np.arange(fine), length, half)
    low = np.arange(kept)
    low[0] = kept
    flip = (-1.0) ** np.arange(half)
    rows = np.stack([wave(low, length, half), wave(np.arange(kept), length, half) * flip])
    return coarse.astype(np.float32), small.astype(np.float32), rows.astype(np.float32)


def split(x):
    hi = x.astype(bf16)
    return hi, (x - hi.astype(f32)).astype(bf16)


def dot(a, b):
    return jnp.dot(a, b, preferred_element_type=f32)


def dot_t(a, b):
    return lax.dot_general(a, b, (((1,), (1,)), ((), ())), preferred_element_type=f32)


def fused_kernel(
    dims, mag_ref, ker_ref, coarse, small, rowt, out_ref,
    acc, mhi, mlo, fs, fr, br, thi, tlo, lhi, llo, kre, kim, kmid, kzero, ahi, alo, z, bhi, blo, wsc,
    mag_sem, k_sem, kmid_sem, zero_send, zero_recv, fsend, frecv, bsend, brecv, out_sem,
):
    n_layer, n_row, n_comp, x_rows, n_y, kept, n_chunk = dims
    devices = n_layer * n_row
    half = n_y // 2
    hrow = n_row // 2
    hdev = devices // 2
    step = half // hdev // 32
    group = 2 * SUB * n_comp
    m_rows = n_layer * group
    n_tile = half // LANE
    l = lax.axis_index("layer")
    r = lax.axis_index("row")
    me = l * n_row + r

    def at(d):
        return (d // n_row, d % n_row)

    barrier = pltpu.get_barrier_semaphore()

    def greet(k, _):
        pl.semaphore_signal(barrier, inc=1, device_id=at((me + k) % devices), device_id_type=MESH)
        return 0

    lax.fori_loop(1, devices, greet, 0)

    def mag_copy(c):
        return pltpu.make_async_copy(mag_ref.at[c, 0], acc.at[c], mag_sem.at[c])

    def k_copy(j):
        src = ker_ref.at[:, pl.ds(pl.multiple_of(j * SUB, SUB), SUB), pl.ds(0, half + LANE)]
        return pltpu.make_async_copy(src, kre.at[:, :, pl.ds(0, half + LANE)], k_sem)

    for c in range(n_comp):
        mag_copy(c).start()
    k_copy(0).start()
    mid_copy = pltpu.make_async_copy(ker_ref.at[:, pl.ds(kept, SUB), pl.ds(0, half + LANE)], kmid, kmid_sem)
    mid_copy.start()
    zero_copy = pltpu.make_async_remote_copy(
        src_ref=ker_ref.at[:, pl.ds(0, SUB), pl.ds(0, half + LANE)], dst_ref=kzero,
        send_sem=zero_send, recv_sem=zero_recv, device_id=at((me + hdev) % devices), device_id_type=MESH,
    )

    sub = lax.broadcasted_iota(jnp.int32, (SUB, half), 0)
    odd_row = jnp.where(sub % 2 == 0, 1.0, -1.0).astype(f32)

    def build_rows(j):
        rows = pl.ds(pl.multiple_of(j * SUB, SUB), SUB)

        def body(e, _):
            c1 = coarse[0, pl.ds(e * step, 1), :]
            s1 = coarse[1, pl.ds(e * step, 1), :]
            for v in range(2):
                c2 = rowt[v, 0, rows, :]
                s2 = rowt[v, 1, rows, :]
                top = c1 * c2 - s1 * s2
                low = -(s1 * c2 + c1 * s2)
                if v == 1:
                    packed = jnp.logical_and(sub == 0, jnp.logical_and(e == 0, j == 0))
                    low = jnp.where(packed, 1.0, low)
                both = jnp.concatenate([top, low], axis=0)
                sign = jnp.concatenate([odd_row, odd_row], axis=0)
                hi, lo = split(both)
                at_row = pl.ds(pl.multiple_of((v * hdev + e) * 2 * SUB, 2 * SUB), 2 * SUB)
                lhi[at_row, 0:half] = hi
                llo[at_row, 0:half] = lo
                lhi[at_row, half : 2 * half] = (hi.astype(f32) * sign).astype(bf16)
                llo[at_row, half : 2 * half] = (lo.astype(f32) * sign).astype(bf16)
            return 0

        lax.fori_loop(0, hdev, body, 0)

    def first(j, _):
        build_rows(j)
        for c in range(n_comp):

            @pl.when(j == 0)
            def _():
                mag_copy(c).wait()

                def body(i, _):
                    rows = pl.ds(pl.multiple_of(i * 16, 16), 16)
                    hi, lo = split(acc[c, rows, :])
                    mhi[c, rows, :] = hi
                    mlo[c, rows, :] = lo
                    return 0

                lax.fori_loop(0, x_rows // 16, body, 0)

            value = dot_t(lhi[...], mhi[c]) + dot_t(llo[...], mhi[c]) + dot_t(lhi[...], mlo[c])
            fs[j, c] = value.reshape(devices, 2 * SUB, x_rows)

            if c == 0:

                @pl.when(j == 0)
                def _():
                    pl.semaphore_wait(barrier, devices - 1)

                    @pl.when(me == 0)
                    def _():
                        zero_copy.start()

            def send(k, _):
                d = (me + k) % devices
                pltpu.make_async_remote_copy(
                    src_ref=fs.at[j, c, d], dst_ref=fr.at[j, c, me], send_sem=fsend.at[j, c], recv_sem=frecv.at[j, c],
                    device_id=at(d), device_id_type=MESH,
                ).start()
                return 0

            lax.fori_loop(1, devices, send, 0)
            fr[j, c, me] = fs[j, c, me]
        return 0

    lax.fori_loop(0, n_chunk, first, 0)

    def build_square(a, _):
        c1 = coarse[0, pl.ds(a, 1), :]
        s1 = coarse[1, pl.ds(a, 1), :]
        for b in range(0, 32, 16):
            c2 = small[0, b : b + 16, :]
            s2 = small[1, b : b + 16, :]
            for v, value in ((0, c1 * c2 - s1 * s2), (1, s1 * c2 + c1 * s2)):
                hi, lo = split(value)
                rows = pl.ds(pl.multiple_of(v * half + a * 32 + b, 16), 16)
                thi[rows, :] = hi
                tlo[rows, :] = lo
        return 0

    lax.fori_loop(0, half // 32, build_square, 0)

    width = half + LANE
    wide_sub = lax.broadcasted_iota(jnp.int32, (SUB, width), 0)
    wide_lane = lax.broadcasted_iota(jnp.int32, (SUB, width), 1)
    lane = lax.broadcasted_iota(jnp.int32, (SUB, LANE), 1)
    lane_sign = jnp.where(lane % 2 == 0, 1.0, -1.0).astype(f32)
    edge = jnp.logical_or(wide_lane == 0, wide_lane == half)
    scale = jnp.where(edge, -1.0, -2.0) * (1.0 / (n_y * n_y))
    wide = (lax.broadcasted_iota(jnp.int32, (1, x_rows), 1) % 2).astype(f32) * -2.0 + 1.0
    mid_copy.wait()

    @pl.when(me == 0)
    def _():
        zero_copy.wait_send()

    @pl.when(me == hdev)
    def _():
        zero_copy.wait_recv()

    def all_of(buf, sem_s, sem_r):
        return pltpu.make_async_remote_copy(
            src_ref=buf, dst_ref=buf, send_sem=sem_s, recv_sem=sem_r,
            device_id=at((me + 1) % devices), device_id_type=MESH,
        )

    def second(j, _):
        top = jnp.logical_and(wide_sub == 0, j == 0)
        use_mid = jnp.logical_and(top, me < hdev)
        use_zero = jnp.logical_and(top, me == hdev)
        wsc[...] = jnp.where(use_zero, scale, 2.0 * scale)
        k_copy(j).wait()

        def prep(i, _):
            w = wsc[...]
            value = jnp.where(use_mid, kmid[i], kre[i, :, 0:width])
            other = jnp.where(use_zero, kzero[i], value)
            for ref, k in ((kre, value * w), (kim, other * w)):
                ref[i, :, 0:width] = k
                ref[i, :, width : width + LANE] = jnp.where(lane == 0, k[:, half:width], k[:, 0:LANE])
            return 0

        lax.fori_loop(0, kre.shape[0], prep, 0)

        for c in range(n_comp):
            all_of(fs.at[j, c, pl.ds(0, devices - 1)], fsend.at[j, c], frecv.at[j, c]).wait_send()
        for c in range(n_comp):
            all_of(fr.at[j, c, pl.ds(0, devices - 1)], fsend.at[j, c], frecv.at[j, c]).wait_recv()

        for h in range(2):
            for s in range(n_layer):
                for c in range(n_comp):
                    row = h * m_rows + s * group + c * 2 * SUB
                    for q in range(hrow):
                        hi, lo = split(fr[j, c, s * n_row + h * hrow + q])
                        ahi[row : row + 2 * SUB, q * x_rows : (q + 1) * x_rows] = hi
                        alo[row : row + 2 * SUB, q * x_rows : (q + 1) * x_rows] = lo

        lane2 = lax.broadcasted_iota(jnp.int32, (1, 256), 1)
        sign2 = jnp.where(lane2 % 2 == 0, 1.0, -1.0).astype(f32)

        def along(n, _):
            cols = pl.ds(pl.multiple_of(n * 256, 256), 256)
            for v in range(2):
                rows = pl.ds(v * half, half)
                p = dot(ahi[...], thi[rows, cols]) + dot(alo[...], thi[rows, cols]) + dot(ahi[...], tlo[rows, cols])
                z[v, :, cols] = p[:m_rows] + sign2 * p[m_rows:]
            return 0

        lax.fori_loop(0, half // 256, along, 0)

        def nyquist(i, _):
            lo_rows = pl.ds(pl.multiple_of(i * 2 * SUB, 2 * SUB), 2 * SUB)
            hi_rows = pl.ds(pl.multiple_of(m_rows + i * 2 * SUB, 2 * SUB), 2 * SUB)
            a = ahi[lo_rows, :].astype(f32) + alo[lo_rows, :].astype(f32)
            b = ahi[hi_rows, :].astype(f32) + alo[hi_rows, :].astype(f32)
            both = a + b
            signs = lax.broadcasted_iota(jnp.int32, both.shape, 1) % 2
            total = jnp.sum(jnp.where(signs == 0, both, -both), axis=1, keepdims=True)
            old = z[1, lo_rows, 0:LANE]
            first_lane = lax.broadcasted_iota(jnp.int32, old.shape, 1) == 0
            z[1, lo_rows, 0:LANE] = jnp.where(first_lane, total, old)
            return 0

        lax.fori_loop(0, m_rows // (2 * SUB), nyquist, 0)

        def point(t, _):
            cols = pl.ds(pl.multiple_of(t * LANE, LANE), LANE)
            side = pl.ds(pl.multiple_of(jnp.where(t == 0, n_tile + 1, t) * LANE, LANE), LANE)
            for target in range(n_layer):
                total = None
                for s in range(n_layer):
                    o = (target - s + n_layer - 1) * 6

                    def k(part, v, ri):
                        return (kre, kim)[ri][o + part, :, (cols, side)[v]]

                    def zz(v, c, ri):
                        row = s * group + c * 2 * SUB + ri * SUB
                        return z[v, row : row + SUB, cols]

                    x = [[[zz(v, c, ri) for ri in range(2)] for c in range(3)] for v in range(2)]
                    diag = [[[k(c, v, ri) for ri in range(2)] for v in range(2)] for c in range(3)]
                    k3 = k(3, 0, 0)
                    k4 = [k(4, 0, 0), k(4, 0, 1)]
                    k5 = [k(5, 0, 0), k(5, 1, 0)]
                    new = []
                    for v in range(2):
                        g = -1.0 if v else 1.0
                        w = 1 - v
                        own, opp = x[v], x[w]
                        swap = ((1.0, 1), (-1.0, 0))
                        for ri in range(2):
                            sg, rj = swap[ri]
                            b3 = (g * sg) * k3 if g * sg < 0 else k3
                            b4 = -k4[ri] if v else k4[ri]
                            b5 = -k5[v] if ri == 0 else k5[v]
                            new.append(diag[0][v][ri] * own[0][ri] + b3 * opp[1][rj] + b4 * opp[2][ri])
                            new.append(b3 * opp[0][rj] + diag[1][v][ri] * own[1][ri] + b5 * own[2][rj])
                            new.append(b4 * opp[0][ri] + b5 * own[1][rj] + diag[2][v][ri] * own[2][ri])
                    total = new if total is None else [a + b for a, b in zip(total, new)]
                for v in range(2):
                    out_cols = pl.ds(pl.multiple_of(v * half + t * LANE, LANE), LANE)
                    for c in range(3):
                        both = jnp.concatenate([total[v * 6 + c], total[v * 6 + 3 + c]], axis=0)
                        hi, lo = split(both)
                        sg = jnp.concatenate([lane_sign, lane_sign], axis=0)
                        row = target * group + c * 2 * SUB
                        for h in range(2):
                            rows = pl.ds(h * m_rows + row, 2 * SUB)
                            bhi[rows, out_cols] = hi if h == 0 else (hi.astype(f32) * sg).astype(bf16)
                            blo[rows, out_cols] = lo if h == 0 else (lo.astype(f32) * sg).astype(bf16)
            return 0

        lax.fori_loop(0, n_tile, point, 0)

        @pl.when(j < n_chunk - 1)
        def _():
            k_copy(j + 1).start()

        def back(q, _):
            cols = pl.ds(pl.multiple_of(q * x_rows, x_rows), x_rows)
            p = dot(bhi[...], thi[:, cols]) + dot(blo[...], thi[:, cols]) + dot(bhi[...], tlo[:, cols])
            edge_col = bhi[:, half : half + LANE].astype(f32) + blo[:, half : half + LANE].astype(f32)
            p = p + edge_col[:, 0:1] * wide
            for h in range(2):
                for target in range(n_layer):
                    for c in range(n_comp):
                        row = h * m_rows + target * group + c * 2 * SUB
                        fs[j, c, target * n_row + h * hrow + q] = p[row : row + 2 * SUB]

            def send(k, _):
                c = k // (2 * n_layer)
                d = (k % n_layer) * n_row + (k // n_layer % 2) * hrow + q

                @pl.when(d != me)
                def _():
                    pltpu.make_async_remote_copy(
                        src_ref=fs.at[j, c, d], dst_ref=br.at[j, c, me], send_sem=bsend.at[j, c], recv_sem=brecv.at[j, c],
                        device_id=at(d), device_id_type=MESH,
                    ).start()

                return 0

            lax.fori_loop(0, n_comp * 2 * n_layer, send, 0)
            return 0

        lax.fori_loop(0, hrow, back, 0)
        for c in range(n_comp):
            br[j, c, me] = fs[j, c, me]
        return 0

    lax.fori_loop(0, n_chunk, second, 0)

    def third(j, _):
        build_rows(j)
        for c in range(n_comp):
            all_of(br.at[j, c, pl.ds(0, devices - 1)], bsend.at[j, c], brecv.at[j, c]).wait_recv()
            turned = jnp.transpose(br[j, c].reshape(devices * 2 * SUB, x_rows))
            hi, lo = split(turned)
            mhi[c, :, 0 : devices * 2 * SUB] = hi
            mlo[c, :, 0 : devices * 2 * SUB] = lo

            def part(n, _):
                cols = pl.ds(pl.multiple_of(n * 512, 512), 512)
                hi = mhi[c, :, 0 : devices * 2 * SUB]
                lo = mlo[c, :, 0 : devices * 2 * SUB]
                value = dot(hi, lhi[:, cols]) + dot(lo, lhi[:, cols]) + dot(hi, llo[:, cols])

                @pl.when(j == 0)
                def _():
                    acc[c, :, cols] = value

                @pl.when(j > 0)
                def _():
                    acc[c, :, cols] = acc[c, :, cols] + value

                return 0

            lax.fori_loop(0, n_y // 512, part, 0)

            @pl.when(j == n_chunk - 1)
            def _():
                pltpu.make_async_copy(acc.at[c], out_ref.at[c, 0], out_sem.at[c]).start()

        return 0

    lax.fori_loop(0, n_chunk, third, 0)
    for j in range(n_chunk):
        for c in range(n_comp):
            all_of(fs.at[j, c, pl.ds(0, devices - 1)], bsend.at[j, c], brecv.at[j, c]).wait_send()
    for c in range(n_comp):
        pltpu.make_async_copy(acc.at[c], out_ref.at[c, 0], out_sem.at[c]).wait()


def fused(magnet, kernel):
    n_layer = lax.axis_size("layer")
    n_row = lax.axis_size("row")
    devices = n_row * n_layer
    n_comp, _, x_rows, n_y = magnet.shape
    n_off, n_part, block, n_x = kernel.shape
    kept = block // 2
    n_chunk = kept // SUB
    half = n_y // 2
    tables = base_tables(block, kept, devices, n_y)
    group = 2 * SUB * n_comp
    m_rows = n_layer * group
    blocks = (n_chunk, n_comp, devices, 2 * SUB, x_rows)
    vm, sem = pltpu.VMEM, pltpu.SemaphoreType.DMA
    width = half + LANE
    n_k = n_off * n_part
    scratch = [
        vm((n_comp, x_rows, n_y), f32),
        vm((n_comp, x_rows, n_y), bf16), vm((n_comp, x_rows, n_y), bf16),
        vm(blocks, f32), vm(blocks, f32), vm(blocks, f32),
        vm((n_y, half), bf16), vm((n_y, half), bf16),
        vm((devices * 2 * SUB, n_y), bf16), vm((devices * 2 * SUB, n_y), bf16),
        vm((n_k, SUB, width + LANE), f32), vm((n_k, SUB, width + LANE), f32),
        vm((n_k, SUB, width), f32), vm((n_k, SUB, width), f32),
        vm((2 * m_rows, half), bf16), vm((2 * m_rows, half), bf16),
        vm((2, m_rows, half), f32),
        vm((2 * m_rows, n_y), bf16), vm((2 * m_rows, n_y), bf16),
        vm((SUB, width), f32),
        sem((n_comp,)), sem, sem, sem, sem,
        *[sem((n_chunk, n_comp))] * 4, sem((n_comp,)),
    ]
    dims = (n_layer, n_row, n_comp, x_rows, n_y, kept, n_chunk)
    anywhere = pl.BlockSpec(memory_space=pl.ANY)
    return pl.pallas_call(
        functools.partial(fused_kernel, dims),
        out_shape=jax.ShapeDtypeStruct(magnet.shape, f32),
        in_specs=[anywhere, anywhere] + [pl.BlockSpec(memory_space=pltpu.VMEM)] * 3,
        out_specs=anywhere,
        scratch_shapes=scratch,
        compiler_params=pltpu.CompilerParams(
            collective_id=0, has_side_effects=True, vmem_limit_bytes=67043328
        ),
    )(magnet, kernel.reshape(n_k, block, n_x), *[jnp.asarray(t) for t in tables])


def fits(magnet, kernel):
    n_layer = lax.axis_size("layer")
    n_row = lax.axis_size("row")
    x_rows, n_y = magnet.shape[2:]
    block, n_x = kernel.shape[2:]
    return (
        n_x == n_y and n_x // 2 % 512 == 0 and x_rows % 256 == 0 and n_row % 2 == 0
        and block % 32 == 0 and x_rows * n_row == n_x and kernel.shape[0] == 2 * n_layer - 1
    )


def local(magnet, kernel):
    if fits(magnet, kernel):
        return fused(magnet, kernel)
    return general(magnet, kernel)


def solution(mesh):
    in_specs = (P(None, "layer", "row", None), P(None, None, ("layer", "row"), None))
    out_specs = P(None, "layer", "row", None)
    return jax.shard_map(local, mesh=mesh, in_specs=in_specs, out_specs=out_specs, check_vma=False)
```

```python
import functools
import math

import jax
import jax.numpy as jnp
import numpy as np
from jax import lax
from jax.experimental import pallas as pl
from jax.experimental.pallas import tpu as pltpu
from jax.sharding import PartitionSpec as P

MESH = pl.DeviceIdType.MESH
SUB, LANE = 8, 128
bf16, f32 = jnp.bfloat16, jnp.float32

high = lax.Precision.HIGH


def phases(left, right, length):
    product = left[:, None] * right[None, :] % length
    theta = product.astype(jnp.float32) * (2.0 * math.pi / length)
    return jnp.cos(theta), jnp.sin(theta)


def product_table(length):
    fine = 32
    idx = jnp.arange(length, dtype=jnp.int32)
    c1, s1 = phases(jnp.arange(length // fine, dtype=jnp.int32) * fine, idx, length)
    c2, s2 = phases(jnp.arange(fine, dtype=jnp.int32), idx, length)
    c1, s1 = c1[:, None], s1[:, None]
    cos = (c1 * c2 - s1 * s2).reshape(length, length)
    sin = (c1 * s2 + s1 * c2).reshape(length, length)
    return cos, sin


def row_table(devices, block, kept, length):
    idx = jnp.arange(length, dtype=jnp.int32)
    c1, s1 = phases(jnp.arange(devices, dtype=jnp.int32) * block, idx, length)
    c2, s2 = phases(jnp.arange(kept, dtype=jnp.int32), idx, length)
    c1, s1 = c1[:, None], s1[:, None]
    pair = jnp.stack([c1 * c2 - s1 * s2, -(c1 * s2 + s1 * c2)], axis=1)
    return pair.reshape(devices * 2 * kept, length)


def general(magnet, kernel):
    n_layer = lax.axis_size("layer")
    n_row = lax.axis_size("row")
    devices = n_row * n_layer
    n_comp, _, x_rows, y_cells = magnet.shape
    block, height = kernel.shape[2], kernel.shape[3]
    kept = block // 2 + 1
    axes = ("layer", "row")

    table = row_table(devices, block, kept, y_cells)
    cos, sin = product_table(height)

    def dot(form, a, b):
        return jnp.einsum(form, a, b, precision=high)

    spec_r, spec_i = [], []
    for c in range(n_comp):
        rows = dot("qy,xy->qx", table, magnet[c, 0])
        moved = lax.all_to_all(
            rows.reshape(devices, 2 * kept, x_rows), axes, split_axis=0, concat_axis=0, tiled=True
        )
        split = moved.reshape(n_layer, n_row, 2, kept, x_rows)
        flat = jnp.transpose(split, (2, 0, 3, 1, 4)).reshape(2 * n_layer * kept, height)
        by_cos = dot("mx,xp->mp", flat, cos).reshape(2, n_layer, kept, height)
        by_sin = dot("mx,xp->mp", flat, sin).reshape(2, n_layer, kept, height)
        spec_r.append(by_cos[0] + by_sin[1])
        spec_i.append(by_cos[1] - by_sin[0])

    row_idx = jnp.arange(kept, dtype=jnp.int32)
    edge = (row_idx == 0) | (row_idx == kept - 1)
    weight = jnp.where(edge, -1.0, -2.0)[:, None] * (1.0 / (height * y_cells))
    coeffs = kernel[:, :, :kept]

    entries = (
        ((0, False), (3, False), (4, True)),
        ((3, False), (1, False), (5, True)),
        ((4, True), (5, True), (2, False)),
    )
    outs = []
    for c in range(n_comp):
        real_rows, imag_rows = [], []
        for target in range(n_layer):
            total_r, total_i = 0.0, 0.0
            for source in range(n_layer):
                offset = target - source + n_layer - 1
                for c2 in range(n_comp):
                    part, turned = entries[c][c2]
                    k = coeffs[offset, part]
                    re, im = spec_r[c2][source], spec_i[c2][source]
                    if turned:
                        total_r = total_r - k * im
                        total_i = total_i + k * re
                    else:
                        total_r = total_r + k * re
                        total_i = total_i + k * im
            real_rows.append(total_r * weight)
            imag_rows.append(total_i * weight)
        field = jnp.stack([jnp.stack(real_rows), jnp.stack(imag_rows)])
        flat = field.reshape(2 * n_layer * kept, height)
        by_cos = dot("mp,px->mx", flat, cos).reshape(2, n_layer, kept, n_row, x_rows)
        by_sin = dot("mp,px->mx", flat, sin).reshape(2, n_layer, kept, n_row, x_rows)
        cells = jnp.stack([by_cos[0] - by_sin[1], by_cos[1] + by_sin[0]], axis=2)
        cells = jnp.transpose(cells, (0, 3, 2, 1, 4)).reshape(devices, 2 * kept, x_rows)
        back = lax.all_to_all(cells, axes, split_axis=0, concat_axis=0, tiled=True)
        outs.append(dot("qx,qy->xy", back.reshape(devices * 2 * kept, x_rows), table))
    return jnp.stack(outs)[:, None]


def wave(angles, length, half):
    product = np.outer(angles, np.arange(half)) % length
    theta = product * (2.0 * np.pi / length)
    return np.stack([np.cos(theta), np.sin(theta)])


def base_tables(block, kept, devices, length):
    half = length // 2
    fine = 32
    coarse = wave(np.arange(half // fine) * fine, length, half)
    small = wave(np.arange(fine), length, half)
    low = np.arange(kept)
    low[0] = kept
    flip = (-1.0) ** np.arange(half)
    rows = np.stack([wave(low, length, half), wave(np.arange(kept), length, half) * flip])
    return coarse.astype(np.float32), small.astype(np.float32), rows.astype(np.float32)


def split(x):
    hi = x.astype(bf16)
    return hi, (x - hi.astype(f32)).astype(bf16)


def dot(a, b):
    return jnp.dot(a, b, preferred_element_type=f32)


def dot_t(a, b):
    return lax.dot_general(a, b, (((1,), (1,)), ((), ())), preferred_element_type=f32)


def fused_kernel(
    dims, mag_ref, ker_ref, coarse_ref, small_ref, rowt_ref, acc,
    coarse, small, rowt, mhi, mlo, fs, fr, br, thi, tlo, lhi, llo, kre, kim, kmid, kzero, ahi, alo, z, bhi, blo, wsc,
    mag_sem, tab_sem, k_sem, kmid_sem, zero_send, zero_recv, fsend, frecv, bsend, brecv,
):
    n_layer, n_row, n_comp, x_rows, n_y, kept, n_chunk = dims
    devices = n_layer * n_row
    half = n_y // 2
    hrow = n_row // 2
    hdev = devices // 2
    step = half // hdev // 32
    group = 2 * SUB * n_comp
    m_rows = n_layer * group
    n_tile = half // LANE
    l = lax.axis_index("layer")
    r = lax.axis_index("row")
    me = l * n_row + r

    side = r // hrow
    inner = l * hrow + r % hrow
    mine = side * hdev + inner

    def at(d):
        return (d // n_row, d % n_row)

    def place(p):
        return (p % hdev // hrow, p // hdev * hrow + p % hrow)

    barrier = pltpu.get_barrier_semaphore()

    def mag_copy(c):
        return pltpu.make_async_copy(mag_ref.at[c, 0], acc.at[c], mag_sem.at[c])

    def k_copy(j):
        src = ker_ref.at[:, pl.ds(pl.multiple_of(j * SUB, SUB), SUB), pl.ds(0, half + LANE)]
        return pltpu.make_async_copy(src, kre.at[:, :, pl.ds(0, half + LANE)], k_sem)

    tables = ((rowt_ref, rowt), (coarse_ref, coarse), (small_ref, small))
    tab_copies = [pltpu.make_async_copy(src, dst, tab_sem.at[i]) for i, (src, dst) in enumerate(tables)]
    tab_copies[0].start()
    tab_copies[1].start()
    for c in range(n_comp):
        mag_copy(c).start()
    tab_copies[2].start()
    k_copy(0).start()
    mid_copy = pltpu.make_async_copy(ker_ref.at[:, pl.ds(kept, SUB), pl.ds(0, half + LANE)], kmid, kmid_sem)
    mid_copy.start()
    zero_copy = pltpu.make_async_remote_copy(
        src_ref=ker_ref.at[:, pl.ds(0, SUB), pl.ds(0, half + LANE)], dst_ref=kzero,
        send_sem=zero_send, recv_sem=zero_recv, device_id=at((me + hdev) % devices), device_id_type=MESH,
    )

    def greet(k, _):
        pl.semaphore_signal(barrier, inc=1, device_id=at((me + k) % devices), device_id_type=MESH)
        return 0

    lax.fori_loop(1, devices, greet, 0)
    tab_copies[0].wait()
    tab_copies[1].wait()

    sub = lax.broadcasted_iota(jnp.int32, (SUB, half), 0)
    odd_row = jnp.where(sub % 2 == 0, 1.0, -1.0).astype(f32)

    def build_rows(j, h):
        rows = pl.ds(pl.multiple_of(j * SUB, SUB), SUB)

        def body(i, _):
            e = i // hrow * n_row + h * hrow + i % hrow
            c1 = coarse[0, pl.ds(e * step, 1), :]
            s1 = coarse[1, pl.ds(e * step, 1), :]
            for v in range(2):
                c2 = rowt[v, 0, rows, :]
                s2 = rowt[v, 1, rows, :]
                top = c1 * c2 - s1 * s2
                low = -(s1 * c2 + c1 * s2)
                if v == 1:
                    packed = jnp.logical_and(sub == 0, jnp.logical_and(e == 0, j == 0))
                    low = jnp.where(packed, 1.0, low)
                both = jnp.concatenate([top, low], axis=0)
                sign = jnp.concatenate([odd_row, odd_row], axis=0)
                hi, lo = split(both)
                p = h * hdev + v * (hdev // 2) + i
                at_row = pl.ds(pl.multiple_of(p * 2 * SUB, 2 * SUB), 2 * SUB)
                lhi[at_row, 0:half] = hi
                llo[at_row, 0:half] = lo
                lhi[at_row, half : 2 * half] = (hi.astype(f32) * sign).astype(bf16)
                llo[at_row, half : 2 * half] = (lo.astype(f32) * sign).astype(bf16)
            return 0

        lax.fori_loop(0, hdev // 2, body, 0)

    def half_rows(h):
        return pl.ds(pl.multiple_of(h * hdev * 2 * SUB, hdev * 2 * SUB), hdev * 2 * SUB)

    def push(src, dst, j, c, h, ssem, rsem):
        def send(k, _):
            p = h * hdev + (inner + k) % hdev

            @pl.when(p != mine)
            def _():
                pltpu.make_async_remote_copy(
                    src_ref=src.at[j, c, p], dst_ref=dst.at[j, c, mine],
                    send_sem=ssem.at[j, c, h], recv_sem=rsem.at[j, c, side],
                    device_id=place(p), device_id_type=MESH,
                ).start()

            return 0

        lax.fori_loop(0, hdev, send, 0)

    def first(j, _):
        for near in range(2):
            h = (side + 1 + near) % 2
            build_rows(j, h)
            for c in range(n_comp):
                if near == 0:

                    @pl.when(j == 0)
                    def _():
                        mag_copy(c).wait()

                        def body(i, _):
                            rows = pl.ds(pl.multiple_of(i * 16, 16), 16)
                            hi, lo = split(acc[c, rows, :])
                            mhi[c, rows, :] = hi
                            mlo[c, rows, :] = lo
                            return 0

                        lax.fori_loop(0, x_rows // 16, body, 0)

                rows = half_rows(h)
                value = dot_t(lhi[rows, :], mhi[c]) + dot_t(llo[rows, :], mhi[c]) + dot_t(lhi[rows, :], mlo[c])
                fs[j, c, pl.ds(h * hdev, hdev)] = value.reshape(hdev, 2 * SUB, x_rows)

                if c == 0 and near == 0:

                    @pl.when(j == 0)
                    def _():
                        pl.semaphore_wait(barrier, devices - 1)

                push(fs, fr, j, c, h, fsend, frecv)
        for c in range(n_comp):
            fr[j, c, mine] = fs[j, c, mine]
        return 0

    lax.fori_loop(0, n_chunk, first, 0)

    @pl.when(me == 0)
    def _():
        zero_copy.start()

    tab_copies[2].wait()

    def build_square(a, _):
        c1 = coarse[0, pl.ds(a, 1), :]
        s1 = coarse[1, pl.ds(a, 1), :]
        for b in range(0, 32, 16):
            c2 = small[0, b : b + 16, :]
            s2 = small[1, b : b + 16, :]
            for v, value in ((0, c1 * c2 - s1 * s2), (1, s1 * c2 + c1 * s2)):
                hi, lo = split(value)
                rows = pl.ds(pl.multiple_of(v * half + a * 32 + b, 16), 16)
                thi[rows, :] = hi
                tlo[rows, :] = lo
        return 0

    lax.fori_loop(0, half // 32, build_square, 0)

    width = half + LANE
    wide_sub = lax.broadcasted_iota(jnp.int32, (SUB, width), 0)
    wide_lane = lax.broadcasted_iota(jnp.int32, (SUB, width), 1)
    lane = lax.broadcasted_iota(jnp.int32, (SUB, LANE), 1)
    lane_sign = jnp.where(lane % 2 == 0, 1.0, -1.0).astype(f32)
    edge = jnp.logical_or(wide_lane == 0, wide_lane == half)
    scale = jnp.where(edge, -1.0, -2.0) * (1.0 / (n_y * n_y))
    wide = (lax.broadcasted_iota(jnp.int32, (1, x_rows), 1) % 2).astype(f32) * -2.0 + 1.0
    mid_copy.wait()

    @pl.when(me == 0)
    def _():
        zero_copy.wait_send()

    @pl.when(me == hdev)
    def _():
        zero_copy.wait_recv()

    def blocks_of(buf, j, c, h, ssem, rsem):
        count = hdev - 1 if isinstance(h, str) else hdev
        k = side if isinstance(h, str) else h
        part = buf.at[j, c, pl.ds(0, count)]
        return pltpu.make_async_remote_copy(
            src_ref=part, dst_ref=part, send_sem=ssem.at[j, c, k], recv_sem=rsem.at[j, c, k],
            device_id=place((mine + 1) % devices), device_id_type=MESH,
        )

    far = 1 - side

    def second(j, _):
        top = jnp.logical_and(wide_sub == 0, j == 0)
        use_mid = jnp.logical_and(top, me < hdev)
        use_zero = jnp.logical_and(top, me == hdev)
        wsc[...] = jnp.where(use_zero, scale, 2.0 * scale)
        k_copy(j).wait()

        def prep(i, _):
            w = wsc[...]
            value = jnp.where(use_mid, kmid[i], kre[i, :, 0:width])
            other = jnp.where(use_zero, kzero[i], value)
            for ref, k in ((kre, value * w), (kim, other * w)):
                ref[i, :, 0:width] = k
                ref[i, :, width : width + LANE] = jnp.where(lane == 0, k[:, half:width], k[:, 0:LANE])
            return 0

        lax.fori_loop(0, kre.shape[0], prep, 0)

        for c in range(n_comp):
            for h in ("near", far):
                blocks_of(fr, j, c, h, fsend, frecv).wait()

        for h in range(2):
            for s in range(n_layer):
                for c in range(n_comp):
                    row = h * m_rows + s * group + c * 2 * SUB
                    for q in range(hrow):
                        hi, lo = split(fr[j, c, h * hdev + s * hrow + q])
                        ahi[row : row + 2 * SUB, q * x_rows : (q + 1) * x_rows] = hi
                        alo[row : row + 2 * SUB, q * x_rows : (q + 1) * x_rows] = lo

        lane2 = lax.broadcasted_iota(jnp.int32, (1, 256), 1)
        sign2 = jnp.where(lane2 % 2 == 0, 1.0, -1.0).astype(f32)

        def along(n, _):
            cols = pl.ds(pl.multiple_of(n * 256, 256), 256)
            for v in range(2):
                rows = pl.ds(v * half, half)
                p = dot(ahi[...], thi[rows, cols]) + dot(alo[...], thi[rows, cols]) + dot(ahi[...], tlo[rows, cols])
                z[v, :, cols] = p[:m_rows] + sign2 * p[m_rows:]
            return 0

        lax.fori_loop(0, half // 256, along, 0)

        def nyquist(i, _):
            lo_rows = pl.ds(pl.multiple_of(i * 2 * SUB, 2 * SUB), 2 * SUB)
            hi_rows = pl.ds(pl.multiple_of(m_rows + i * 2 * SUB, 2 * SUB), 2 * SUB)
            a = ahi[lo_rows, :].astype(f32) + alo[lo_rows, :].astype(f32)
            b = ahi[hi_rows, :].astype(f32) + alo[hi_rows, :].astype(f32)
            both = a + b
            signs = lax.broadcasted_iota(jnp.int32, both.shape, 1) % 2
            total = jnp.sum(jnp.where(signs == 0, both, -both), axis=1, keepdims=True)
            old = z[1, lo_rows, 0:LANE]
            first_lane = lax.broadcasted_iota(jnp.int32, old.shape, 1) == 0
            z[1, lo_rows, 0:LANE] = jnp.where(first_lane, total, old)
            return 0

        lax.fori_loop(0, m_rows // (2 * SUB), nyquist, 0)

        def point(t, _):
            cols = pl.ds(pl.multiple_of(t * LANE, LANE), LANE)
            corner = pl.ds(pl.multiple_of(jnp.where(t == 0, n_tile + 1, t) * LANE, LANE), LANE)
            for target in range(n_layer):
                total = None
                for s in range(n_layer):
                    o = (target - s + n_layer - 1) * 6

                    def k(part, v, ri):
                        return (kre, kim)[ri][o + part, :, (cols, corner)[v]]

                    def zz(v, c, ri):
                        row = s * group + c * 2 * SUB + ri * SUB
                        return z[v, row : row + SUB, cols]

                    x = [[[zz(v, c, ri) for ri in range(2)] for c in range(3)] for v in range(2)]
                    diag = [[[k(c, v, ri) for ri in range(2)] for v in range(2)] for c in range(3)]
                    k3 = k(3, 0, 0)
                    k4 = [k(4, 0, 0), k(4, 0, 1)]
                    k5 = [k(5, 0, 0), k(5, 1, 0)]
                    new = []
                    for v in range(2):
                        g = -1.0 if v else 1.0
                        w = 1 - v
                        own, opp = x[v], x[w]
                        swap = ((1.0, 1), (-1.0, 0))
                        for ri in range(2):
                            sg, rj = swap[ri]
                            b3 = (g * sg) * k3 if g * sg < 0 else k3
                            b4 = -k4[ri] if v else k4[ri]
                            b5 = -k5[v] if ri == 0 else k5[v]
                            new.append(diag[0][v][ri] * own[0][ri] + b3 * opp[1][rj] + b4 * opp[2][ri])
                            new.append(b3 * opp[0][rj] + diag[1][v][ri] * own[1][ri] + b5 * own[2][rj])
                            new.append(b4 * opp[0][ri] + b5 * own[1][rj] + diag[2][v][ri] * own[2][ri])
                    total = new if total is None else [a + b for a, b in zip(total, new)]
                for v in range(2):
                    out_cols = pl.ds(pl.multiple_of(v * half + t * LANE, LANE), LANE)
                    for c in range(3):
                        both = jnp.concatenate([total[v * 6 + c], total[v * 6 + 3 + c]], axis=0)
                        hi, lo = split(both)
                        sg = jnp.concatenate([lane_sign, lane_sign], axis=0)
                        row = target * group + c * 2 * SUB
                        for h in range(2):
                            rows = pl.ds(h * m_rows + row, 2 * SUB)
                            bhi[rows, out_cols] = hi if h == 0 else (hi.astype(f32) * sg).astype(bf16)
                            blo[rows, out_cols] = lo if h == 0 else (lo.astype(f32) * sg).astype(bf16)
            return 0

        lax.fori_loop(0, n_tile, point, 0)

        @pl.when(j < n_chunk - 1)
        def _():
            k_copy(j + 1).start()

        def back(q, _):
            cols = pl.ds(pl.multiple_of(q * x_rows, x_rows), x_rows)
            p = dot(bhi[...], thi[:, cols]) + dot(blo[...], thi[:, cols]) + dot(bhi[...], tlo[:, cols])
            edge_col = bhi[:, half : half + LANE].astype(f32) + blo[:, half : half + LANE].astype(f32)
            p = p + edge_col[:, 0:1] * wide
            for h in range(2):
                for target in range(n_layer):
                    for c in range(n_comp):
                        row = h * m_rows + target * group + c * 2 * SUB
                        fs[j, c, h * hdev + target * hrow + q] = p[row : row + 2 * SUB]

            return 0

        lax.fori_loop(0, hrow, back, 0)
        for h in (side, far):
            for c in range(n_comp):
                push(fs, br, j, c, h, bsend, brecv)
        for c in range(n_comp):
            br[j, c, mine] = fs[j, c, mine]
        return 0

    lax.fori_loop(0, n_chunk, second, 0)

    def third(j, _):
        for h in range(2):
            build_rows(j, h)
        depth = hdev * 2 * SUB
        for name, h in (("near", side), (far, far)):
            rows = half_rows(h)
            for c in range(n_comp):
                blocks_of(br, j, c, name, bsend, brecv).wait_recv()
                turned = jnp.transpose(br[j, c, pl.ds(h * hdev, hdev)].reshape(depth, x_rows))
                hi, lo = split(turned)
                mhi[c, :, 0:depth] = hi
                mlo[c, :, 0:depth] = lo

                def part(n, _):
                    cols = pl.ds(pl.multiple_of(n * 512, 512), 512)
                    hi = mhi[c, :, 0:depth]
                    lo = mlo[c, :, 0:depth]
                    value = dot(hi, lhi[rows, cols]) + dot(lo, lhi[rows, cols]) + dot(hi, llo[rows, cols])
                    if name == "near":

                        @pl.when(j == 0)
                        def _():
                            acc[c, :, cols] = value

                        @pl.when(j > 0)
                        def _():
                            acc[c, :, cols] = acc[c, :, cols] + value

                    else:
                        acc[c, :, cols] = acc[c, :, cols] + value
                    return 0

                lax.fori_loop(0, n_y // 512, part, 0)
        return 0

    lax.fori_loop(0, n_chunk, third, 0)
    for j in range(n_chunk):
        for c in range(n_comp):
            for h in ("near", far):
                blocks_of(fs, j, c, h, bsend, brecv).wait_send()


def fused(magnet, kernel):
    n_layer = lax.axis_size("layer")
    n_row = lax.axis_size("row")
    devices = n_row * n_layer
    n_comp, _, x_rows, n_y = magnet.shape
    n_off, n_part, block, n_x = kernel.shape
    kept = block // 2
    n_chunk = kept // SUB
    half = n_y // 2
    tables = base_tables(block, kept, devices, n_y)
    group = 2 * SUB * n_comp
    m_rows = n_layer * group
    blocks = (n_chunk, n_comp, devices, 2 * SUB, x_rows)
    vm, sem = pltpu.VMEM, pltpu.SemaphoreType.DMA
    width = half + LANE
    n_k = n_off * n_part
    scratch = [
        *[vm(t.shape, f32) for t in tables],
        vm((n_comp, x_rows, n_y), bf16), vm((n_comp, x_rows, n_y), bf16),
        vm(blocks, f32), vm(blocks, f32), vm(blocks, f32),
        vm((n_y, half), bf16), vm((n_y, half), bf16),
        vm((devices * 2 * SUB, n_y), bf16), vm((devices * 2 * SUB, n_y), bf16),
        vm((n_k, SUB, width + LANE), f32), vm((n_k, SUB, width + LANE), f32),
        vm((n_k, SUB, width), f32), vm((n_k, SUB, width), f32),
        vm((2 * m_rows, half), bf16), vm((2 * m_rows, half), bf16),
        vm((2, m_rows, half), f32),
        vm((2 * m_rows, n_y), bf16), vm((2 * m_rows, n_y), bf16),
        vm((SUB, width), f32),
        sem((n_comp,)), sem((3,)), sem, sem, sem, sem,
        *[sem((n_chunk, n_comp, 2))] * 4,
    ]
    dims = (n_layer, n_row, n_comp, x_rows, n_y, kept, n_chunk)
    anywhere = pl.BlockSpec(memory_space=pl.ANY)
    return pl.pallas_call(
        functools.partial(fused_kernel, dims),
        out_shape=pltpu.VMEM((n_comp, x_rows, n_y), f32),
        in_specs=[anywhere] * 5,
        out_specs=pl.BlockSpec(memory_space=pltpu.VMEM),
        scratch_shapes=scratch,
        compiler_params=pltpu.CompilerParams(
            collective_id=0, has_side_effects=True, vmem_limit_bytes=54 * 2**20
        ),
    )(magnet, kernel.reshape(n_k, block, n_x), *[jnp.asarray(t) for t in tables]).reshape(magnet.shape)


def fits(magnet, kernel):
    n_layer = lax.axis_size("layer")
    n_row = lax.axis_size("row")
    x_rows, n_y = magnet.shape[2:]
    block, n_x = kernel.shape[2:]
    return (
        n_x == n_y and n_x // 2 % 512 == 0 and x_rows % 256 == 0 and n_row % 2 == 0
        and n_layer % 2 == 0 and block % 32 == 0 and x_rows * n_row == n_x and kernel.shape[0] == 2 * n_layer - 1
    )


def local(magnet, kernel):
    if fits(magnet, kernel):
        return fused(magnet, kernel)
    return general(magnet, kernel)


def solution(mesh):
    in_specs = (P(None, "layer", "row", None), P(None, None, ("layer", "row"), None))
    out_specs = P(None, "layer", "row", None)
    return jax.shard_map(local, mesh=mesh, in_specs=in_specs, out_specs=out_specs, check_vma=False)
```

```python
import functools
import math

import jax
import jax.numpy as jnp
import numpy as np
from jax import lax
from jax.experimental import pallas as pl
from jax.experimental.pallas import tpu as pltpu
from jax.sharding import PartitionSpec as P

MESH = pl.DeviceIdType.MESH
SUB, LANE = 8, 128
bf16, f32 = jnp.bfloat16, jnp.float32

high = lax.Precision.HIGH


def phases(left, right, length):
    product = left[:, None] * right[None, :] % length
    theta = product.astype(jnp.float32) * (2.0 * math.pi / length)
    return jnp.cos(theta), jnp.sin(theta)


def product_table(length):
    fine = 32
    idx = jnp.arange(length, dtype=jnp.int32)
    c1, s1 = phases(jnp.arange(length // fine, dtype=jnp.int32) * fine, idx, length)
    c2, s2 = phases(jnp.arange(fine, dtype=jnp.int32), idx, length)
    c1, s1 = c1[:, None], s1[:, None]
    cos = (c1 * c2 - s1 * s2).reshape(length, length)
    sin = (c1 * s2 + s1 * c2).reshape(length, length)
    return cos, sin


def row_table(devices, block, kept, length):
    idx = jnp.arange(length, dtype=jnp.int32)
    c1, s1 = phases(jnp.arange(devices, dtype=jnp.int32) * block, idx, length)
    c2, s2 = phases(jnp.arange(kept, dtype=jnp.int32), idx, length)
    c1, s1 = c1[:, None], s1[:, None]
    pair = jnp.stack([c1 * c2 - s1 * s2, -(c1 * s2 + s1 * c2)], axis=1)
    return pair.reshape(devices * 2 * kept, length)


def general(magnet, kernel):
    n_layer = lax.axis_size("layer")
    n_row = lax.axis_size("row")
    devices = n_row * n_layer
    n_comp, _, x_rows, y_cells = magnet.shape
    block, height = kernel.shape[2], kernel.shape[3]
    kept = block // 2 + 1
    axes = ("layer", "row")

    table = row_table(devices, block, kept, y_cells)
    cos, sin = product_table(height)

    def dot(form, a, b):
        return jnp.einsum(form, a, b, precision=high)

    spec_r, spec_i = [], []
    for c in range(n_comp):
        rows = dot("qy,xy->qx", table, magnet[c, 0])
        moved = lax.all_to_all(
            rows.reshape(devices, 2 * kept, x_rows), axes, split_axis=0, concat_axis=0, tiled=True
        )
        split = moved.reshape(n_layer, n_row, 2, kept, x_rows)
        flat = jnp.transpose(split, (2, 0, 3, 1, 4)).reshape(2 * n_layer * kept, height)
        by_cos = dot("mx,xp->mp", flat, cos).reshape(2, n_layer, kept, height)
        by_sin = dot("mx,xp->mp", flat, sin).reshape(2, n_layer, kept, height)
        spec_r.append(by_cos[0] + by_sin[1])
        spec_i.append(by_cos[1] - by_sin[0])

    row_idx = jnp.arange(kept, dtype=jnp.int32)
    edge = (row_idx == 0) | (row_idx == kept - 1)
    weight = jnp.where(edge, -1.0, -2.0)[:, None] * (1.0 / (height * y_cells))
    coeffs = kernel[:, :, :kept]

    entries = (
        ((0, False), (3, False), (4, True)),
        ((3, False), (1, False), (5, True)),
        ((4, True), (5, True), (2, False)),
    )
    outs = []
    for c in range(n_comp):
        real_rows, imag_rows = [], []
        for target in range(n_layer):
            total_r, total_i = 0.0, 0.0
            for source in range(n_layer):
                offset = target - source + n_layer - 1
                for c2 in range(n_comp):
                    part, turned = entries[c][c2]
                    k = coeffs[offset, part]
                    re, im = spec_r[c2][source], spec_i[c2][source]
                    if turned:
                        total_r = total_r - k * im
                        total_i = total_i + k * re
                    else:
                        total_r = total_r + k * re
                        total_i = total_i + k * im
            real_rows.append(total_r * weight)
            imag_rows.append(total_i * weight)
        field = jnp.stack([jnp.stack(real_rows), jnp.stack(imag_rows)])
        flat = field.reshape(2 * n_layer * kept, height)
        by_cos = dot("mp,px->mx", flat, cos).reshape(2, n_layer, kept, n_row, x_rows)
        by_sin = dot("mp,px->mx", flat, sin).reshape(2, n_layer, kept, n_row, x_rows)
        cells = jnp.stack([by_cos[0] - by_sin[1], by_cos[1] + by_sin[0]], axis=2)
        cells = jnp.transpose(cells, (0, 3, 2, 1, 4)).reshape(devices, 2 * kept, x_rows)
        back = lax.all_to_all(cells, axes, split_axis=0, concat_axis=0, tiled=True)
        outs.append(dot("qx,qy->xy", back.reshape(devices * 2 * kept, x_rows), table))
    return jnp.stack(outs)[:, None]


def wave(angles, length, half):
    product = np.outer(angles, np.arange(half)) % length
    theta = product * (2.0 * np.pi / length)
    return np.stack([np.cos(theta), np.sin(theta)])


def base_tables(block, kept, devices, length):
    half = length // 2
    fine = 32
    coarse = wave(np.arange(half // fine) * fine, length, half)
    steps = wave(np.arange(devices // 2) * block, length, half)
    small = wave(np.arange(fine), length, half)
    low = np.arange(kept)
    low[0] = kept
    flip = (-1.0) ** np.arange(half)
    rows = np.stack([wave(low, length, half), wave(np.arange(kept), length, half) * flip])
    return [t.astype(np.float32) for t in (coarse, small, steps, rows)]


def split(x):
    hi = x.astype(bf16)
    return hi, (x - hi.astype(f32)).astype(bf16)


def dot(a, b):
    return jnp.dot(a, b, preferred_element_type=f32)


def dot_t(a, b):
    return lax.dot_general(a, b, (((1,), (1,)), ((), ())), preferred_element_type=f32)


def fused_kernel(
    dims, mag_ref, ker_ref, coarse_ref, small_ref, steps_ref, rowt_ref, acc,
    coarse, small, steps, rowt, mhi, mlo, fs, fr, br, thi, tlo, rows_hl, turn_hl, kre, kim, kmid, kzero, ahi, alo, z, bhi, blo, wsc,
    mag_sem, tab_sem, k_sem, kmid_sem, zero_send, zero_recv, fsend, frecv, bsend, brecv,
):
    n_layer, n_row, n_comp, x_rows, n_y, kept, n_chunk = dims
    devices = n_layer * n_row
    half = n_y // 2
    hrow = n_row // 2
    hdev = devices // 2
    group = 2 * SUB * n_comp
    m_rows = n_layer * group
    n_tile = half // LANE
    l = lax.axis_index("layer")
    r = lax.axis_index("row")
    me = l * n_row + r

    side = r // hrow
    inner = l * hrow + r % hrow
    mine = side * hdev + inner

    def at(d):
        return (d // n_row, d % n_row)

    def place(p):
        return (p % hdev // hrow, p // hdev * hrow + p % hrow)

    head, tail = pl.ds(0, SUB), pl.ds(SUB, kept - SUB)
    tables = [
        (steps_ref, steps), (rowt_ref.at[:, :, head], rowt.at[:, :, head]),
        (coarse_ref, coarse), (small_ref, small),
    ]
    if n_chunk > 1:
        tables.append((rowt_ref.at[:, :, tail], rowt.at[:, :, tail]))
    tab_copies = [pltpu.make_async_copy(src, dst, tab_sem.at[i]) for i, (src, dst) in enumerate(tables)]

    def mag_copy(c, i):
        rows = pl.ds(i * (x_rows // 2), x_rows // 2)
        return pltpu.make_async_copy(mag_ref.at[c, 0, rows], acc.at[c, rows], mag_sem.at[c, i])

    def k_copy(j):
        src = ker_ref.at[:, pl.ds(pl.multiple_of(j * SUB, SUB), SUB), pl.ds(0, half + LANE)]
        return pltpu.make_async_copy(src, kre.at[:, :, pl.ds(0, half + LANE)], k_sem)

    mid_copy = pltpu.make_async_copy(ker_ref.at[:, pl.ds(kept, SUB), pl.ds(0, half + LANE)], kmid, kmid_sem)
    zero_copy = pltpu.make_async_remote_copy(
        src_ref=ker_ref.at[:, pl.ds(0, SUB), pl.ds(0, half + LANE)], dst_ref=kzero,
        send_sem=zero_send, recv_sem=zero_recv, device_id=at((me + hdev) % devices), device_id_type=MESH,
    )

    tab_copies[0].start()
    tab_copies[1].start()
    barrier = pltpu.get_barrier_semaphore()
    layers = [(l + i) % n_layer for i in range(n_layer)]
    rows_of = [(r + i) % n_row for i in range(n_row)]
    for i in range(1, devices):
        target = (layers[i // n_row], rows_of[i % n_row])
        pl.semaphore_signal(barrier, inc=1, device_id=target, device_id_type=MESH)
    mag_copy(0, 0).start()
    mag_copy(0, 1).start()
    tab_copies[0].wait()
    tab_copies[1].wait()

    sub = lax.broadcasted_iota(jnp.int32, (SUB, half), 0)
    odd_row = jnp.where(sub % 2 == 0, 1.0, -1.0).astype(f32)

    def build_rows(j, h):
        rows = pl.ds(pl.multiple_of(j * SUB, SUB), SUB)

        def body(i, _):
            e = i // hrow * n_row + h * hrow + i % hrow
            c1 = steps[0, pl.ds(e, 1), :]
            s1 = steps[1, pl.ds(e, 1), :]
            for v in range(2):
                c2 = rowt[v, 0, rows, :]
                s2 = rowt[v, 1, rows, :]
                top = c1 * c2 - s1 * s2
                low = -(s1 * c2 + c1 * s2)
                if v == 1:
                    packed = jnp.logical_and(sub == 0, jnp.logical_and(e == 0, j == 0))
                    low = jnp.where(packed, 1.0, low)
                both = jnp.concatenate([top, low], axis=0)
                sign = jnp.concatenate([odd_row, odd_row], axis=0)
                hi, lo = split(both)
                at_row = pl.ds(pl.multiple_of((v * (hdev // 2) + i) * 2 * SUB, 2 * SUB), 2 * SUB)
                for k, value in enumerate((hi, lo)):
                    rows_hl[h, k, at_row, 0:half] = value
                    rows_hl[h, k, at_row, half : 2 * half] = (value.astype(f32) * sign).astype(bf16)
            return 0

        lax.fori_loop(0, hdev // 2, body, 0)

    depth = hdev * 2 * SUB

    def push(src, dst, j, c, h, ssem, rsem, some=slice(0, x_rows)):
        def send(k, _):
            p = h * hdev + (inner + k) % hdev

            @pl.when(p != mine)
            def _():
                pltpu.make_async_remote_copy(
                    src_ref=src.at[j, c, p, :, some], dst_ref=dst.at[j, c, mine, :, some],
                    send_sem=ssem, recv_sem=rsem,
                    device_id=place(p), device_id_type=MESH,
                ).start()

            return 0

        lax.fori_loop(0, hdev, send, 0)

    def first(j, _):
        @pl.when(j == 1)
        def _():
            for copy in tab_copies[4:]:
                copy.wait()

        for near in range(2):
            h = (side + 1 + near) % 2
            build_rows(j, h)
            if near == 0:

                @pl.when(j == 0)
                def _():
                    for c in range(1, n_comp):
                        mag_copy(c, 0).start()
                        mag_copy(c, 1).start()
                    for copy in tab_copies[2:]:
                        copy.start()

            for c in range(n_comp):
                pieces = 2 if c == 0 and near == 0 else 1
                size = x_rows // pieces
                for i in range(pieces):
                    some = slice(i * size, (i + 1) * size)
                    if near == 0:

                        @pl.when(j == 0)
                        def _():
                            for k in range(2 // pieces):
                                mag_copy(c, i + k).wait()

                            def body(k, _):
                                rows = pl.ds(pl.multiple_of(i * size + k * 16, 16), 16)
                                hi, lo = split(acc[c, rows, :])
                                mhi[c, rows, :] = hi
                                mlo[c, rows, :] = lo
                                return 0

                            lax.fori_loop(0, size // 16, body, 0)

                    value = dot_t(rows_hl[h].reshape(2 * depth, n_y), mhi[c, some])
                    value = value[:depth] + value[depth:] + dot_t(rows_hl[h, 0], mlo[c, some])
                    fs[j, c, pl.ds(h * hdev, hdev), :, some] = value.reshape(hdev, 2 * SUB, size)

                    if c == 0 and near == 0 and i == 0:

                        @pl.when(j == 0)
                        def _():
                            pl.semaphore_wait(barrier, devices - 1)

                    push(fs, fr, j, c, h, fsend.at[j, h], frecv.at[j, side], some)
        for c in range(n_comp):
            fr[j, c, mine] = fs[j, c, mine]
        return 0

    lax.fori_loop(0, n_chunk, first, 0)
    k_copy(0).start()
    mid_copy.start()

    @pl.when(me == 0)
    def _():
        zero_copy.start()

    tab_copies[2].wait()
    tab_copies[3].wait()

    def build_square(a, _):
        c1 = coarse[0, pl.ds(a, 1), :]
        s1 = coarse[1, pl.ds(a, 1), :]
        for b in range(0, 32, 16):
            c2 = small[0, b : b + 16, :]
            s2 = small[1, b : b + 16, :]
            for v, value in ((0, c1 * c2 - s1 * s2), (1, s1 * c2 + c1 * s2)):
                hi, lo = split(value)
                rows = pl.ds(pl.multiple_of(v * half + a * 32 + b, 16), 16)
                thi[rows, :] = hi
                tlo[rows, :] = lo
        return 0

    lax.fori_loop(0, half // 32, build_square, 0)

    width = half + LANE
    wide_sub = lax.broadcasted_iota(jnp.int32, (SUB, width), 0)
    wide_lane = lax.broadcasted_iota(jnp.int32, (SUB, width), 1)
    lane = lax.broadcasted_iota(jnp.int32, (SUB, LANE), 1)
    lane_sign = jnp.where(lane % 2 == 0, 1.0, -1.0).astype(f32)
    edge = jnp.logical_or(wide_lane == 0, wide_lane == half)
    scale = jnp.where(edge, -1.0, -2.0) * (1.0 / (n_y * n_y))
    wide = (lax.broadcasted_iota(jnp.int32, (1, x_rows), 1) % 2).astype(f32) * -2.0 + 1.0
    mid_copy.wait()

    @pl.when(me == 0)
    def _():
        zero_copy.wait_send()

    @pl.when(me == hdev)
    def _():
        zero_copy.wait_recv()

    def blocks_of(buf, j, name, ssem, rsem, c=None):
        blocks = pl.ds(0, hdev - 1 if name == "near" else hdev)
        part = buf.at[j, :, blocks] if c is None else buf.at[j, c, blocks]
        return pltpu.make_async_remote_copy(
            src_ref=part, dst_ref=part, send_sem=ssem, recv_sem=rsem,
            device_id=place((mine + 1) % devices), device_id_type=MESH,
        )

    far = 1 - side

    def second(j, _):
        top = jnp.logical_and(wide_sub == 0, j == 0)
        use_mid = jnp.logical_and(top, me < hdev)
        use_zero = jnp.logical_and(top, me == hdev)
        wsc[...] = jnp.where(use_zero, scale, 2.0 * scale)
        k_copy(j).wait()

        def prep(i, _):
            w = wsc[...]
            value = jnp.where(use_mid, kmid[i], kre[i, :, 0:width])
            other = jnp.where(use_zero, kzero[i], value)
            for ref, k in ((kre, value * w), (kim, other * w)):
                ref[i, :, 0:width] = k
                ref[i, :, width : width + LANE] = jnp.where(lane == 0, k[:, half:width], k[:, 0:LANE])
            return 0

        lax.fori_loop(0, kre.shape[0], prep, 0)

        for name, h in (("near", side), ("far", far)):
            blocks_of(fr, j, name, fsend.at[j, h], frecv.at[j, h]).wait()

        for h in range(2):
            for s in range(n_layer):
                for c in range(n_comp):
                    row = h * m_rows + s * group + c * 2 * SUB
                    for q in range(hrow):
                        hi, lo = split(fr[j, c, h * hdev + s * hrow + q])
                        ahi[row : row + 2 * SUB, q * x_rows : (q + 1) * x_rows] = hi
                        alo[row : row + 2 * SUB, q * x_rows : (q + 1) * x_rows] = lo

        lane2 = lax.broadcasted_iota(jnp.int32, (1, 256), 1)
        sign2 = jnp.where(lane2 % 2 == 0, 1.0, -1.0).astype(f32)

        def along(n, _):
            cols = pl.ds(pl.multiple_of(n * 256, 256), 256)
            for v in range(2):
                rows = pl.ds(v * half, half)
                p = dot(ahi[...], thi[rows, cols]) + dot(alo[...], thi[rows, cols]) + dot(ahi[...], tlo[rows, cols])
                z[v, :, cols] = p[:m_rows] + sign2 * p[m_rows:]
            return 0

        lax.fori_loop(0, half // 256, along, 0)

        def nyquist(i, _):
            lo_rows = pl.ds(pl.multiple_of(i * 2 * SUB, 2 * SUB), 2 * SUB)
            hi_rows = pl.ds(pl.multiple_of(m_rows + i * 2 * SUB, 2 * SUB), 2 * SUB)
            a = ahi[lo_rows, :].astype(f32) + alo[lo_rows, :].astype(f32)
            b = ahi[hi_rows, :].astype(f32) + alo[hi_rows, :].astype(f32)
            both = a + b
            signs = lax.broadcasted_iota(jnp.int32, both.shape, 1) % 2
            total = jnp.sum(jnp.where(signs == 0, both, -both), axis=1, keepdims=True)
            old = z[1, lo_rows, 0:LANE]
            first_lane = lax.broadcasted_iota(jnp.int32, old.shape, 1) == 0
            z[1, lo_rows, 0:LANE] = jnp.where(first_lane, total, old)
            return 0

        lax.fori_loop(0, m_rows // (2 * SUB), nyquist, 0)

        def point(t, _):
            cols = pl.ds(pl.multiple_of(t * LANE, LANE), LANE)
            corner = pl.ds(pl.multiple_of(jnp.where(t == 0, n_tile + 1, t) * LANE, LANE), LANE)
            for target in range(n_layer):
                total = None
                for s in range(n_layer):
                    o = (target - s + n_layer - 1) * 6

                    def k(part, v, ri):
                        return (kre, kim)[ri][o + part, :, (cols, corner)[v]]

                    def zz(v, c, ri):
                        row = s * group + c * 2 * SUB + ri * SUB
                        return z[v, row : row + SUB, cols]

                    x = [[[zz(v, c, ri) for ri in range(2)] for c in range(3)] for v in range(2)]
                    diag = [[[k(c, v, ri) for ri in range(2)] for v in range(2)] for c in range(3)]
                    k3 = k(3, 0, 0)
                    k4 = [k(4, 0, 0), k(4, 0, 1)]
                    k5 = [k(5, 0, 0), k(5, 1, 0)]
                    new = []
                    for v in range(2):
                        g = -1.0 if v else 1.0
                        w = 1 - v
                        own, opp = x[v], x[w]
                        swap = ((1.0, 1), (-1.0, 0))
                        for ri in range(2):
                            sg, rj = swap[ri]
                            b3 = (g * sg) * k3 if g * sg < 0 else k3
                            b4 = -k4[ri] if v else k4[ri]
                            b5 = -k5[v] if ri == 0 else k5[v]
                            new.append(diag[0][v][ri] * own[0][ri] + b3 * opp[1][rj] + b4 * opp[2][ri])
                            new.append(b3 * opp[0][rj] + diag[1][v][ri] * own[1][ri] + b5 * own[2][rj])
                            new.append(b4 * opp[0][ri] + b5 * own[1][rj] + diag[2][v][ri] * own[2][ri])
                    total = new if total is None else [a + b for a, b in zip(total, new)]
                for v in range(2):
                    out_cols = pl.ds(pl.multiple_of(v * half + t * LANE, LANE), LANE)
                    for c in range(3):
                        both = jnp.concatenate([total[v * 6 + c], total[v * 6 + 3 + c]], axis=0)
                        hi, lo = split(both)
                        sg = jnp.concatenate([lane_sign, lane_sign], axis=0)
                        row = target * group + c * 2 * SUB
                        for h in range(2):
                            rows = pl.ds(h * m_rows + row, 2 * SUB)
                            bhi[rows, out_cols] = hi if h == 0 else (hi.astype(f32) * sg).astype(bf16)
                            blo[rows, out_cols] = lo if h == 0 else (lo.astype(f32) * sg).astype(bf16)
            return 0

        lax.fori_loop(0, n_tile, point, 0)

        @pl.when(j < n_chunk - 1)
        def _():
            k_copy(j + 1).start()

        def back(q, _):
            cols = pl.ds(pl.multiple_of(q * x_rows, x_rows), x_rows)
            p = dot(bhi[...], thi[:, cols]) + dot(blo[...], thi[:, cols]) + dot(bhi[...], tlo[:, cols])
            edge_col = bhi[:, half : half + LANE].astype(f32) + blo[:, half : half + LANE].astype(f32)
            p = p + edge_col[:, 0:1] * wide
            for h in range(2):
                for target in range(n_layer):
                    for c in range(n_comp):
                        row = h * m_rows + target * group + c * 2 * SUB
                        fs[j, c, h * hdev + target * hrow + q] = p[row : row + 2 * SUB]

            return 0

        lax.fori_loop(0, hrow, back, 0)
        for h in (side, far):
            for c in range(n_comp):
                push(fs, br, j, c, h, bsend.at[j, h], brecv.at[j, c, side])
        for c in range(n_comp):
            br[j, c, mine] = fs[j, c, mine]
        return 0

    lax.fori_loop(0, n_chunk, second, 0)

    wide_part = n_y // 2

    def third(j, _):
        for h in range(2):
            build_rows(j, h)

        @pl.when(j > 0)
        def _():
            blocks_of(fs, j - 1, "far", bsend.at[j - 1, far], brecv.at[j - 1, 0, far]).wait_send()

        for name, h in (("near", side), ("far", far)):
            for c in range(n_comp):
                blocks_of(br, j, name, bsend.at[j, h], brecv.at[j, c, h], c).wait_recv()
                turned = jnp.transpose(br[j, c, pl.ds(h * hdev, hdev)].reshape(depth, x_rows))
                hi, lo = split(turned)
                turn_hl[0:x_rows, :] = hi
                turn_hl[x_rows : 2 * x_rows, :] = lo

                def part(n, _):
                    cols = pl.ds(pl.multiple_of(n * wide_part, wide_part), wide_part)
                    value = dot(turn_hl[...], rows_hl[h, 0, :, cols])
                    value = value[:x_rows] + value[x_rows:] + dot(turn_hl[0:x_rows, :], rows_hl[h, 1, :, cols])
                    if name == "near":

                        @pl.when(j == 0)
                        def _():
                            acc[c, :, cols] = value

                        @pl.when(j > 0)
                        def _():
                            acc[c, :, cols] = acc[c, :, cols] + value

                    else:
                        acc[c, :, cols] = acc[c, :, cols] + value
                    return 0

                lax.fori_loop(0, n_y // wide_part, part, 0)
            if name == "near":
                blocks_of(fs, j, name, bsend.at[j, h], brecv.at[j, 0, h]).wait_send()
        return 0

    lax.fori_loop(0, n_chunk, third, 0)
    blocks_of(fs, n_chunk - 1, "far", bsend.at[n_chunk - 1, far], brecv.at[n_chunk - 1, 0, far]).wait_send()


def fused(magnet, kernel):
    n_layer = lax.axis_size("layer")
    n_row = lax.axis_size("row")
    devices = n_row * n_layer
    n_comp, _, x_rows, n_y = magnet.shape
    n_off, n_part, block, n_x = kernel.shape
    kept = block // 2
    n_chunk = kept // SUB
    half = n_y // 2
    tables = base_tables(block, kept, devices, n_y)
    group = 2 * SUB * n_comp
    m_rows = n_layer * group
    blocks = (n_chunk, n_comp, devices, 2 * SUB, x_rows)
    vm, sem = pltpu.VMEM, pltpu.SemaphoreType.DMA
    width = half + LANE
    n_k = n_off * n_part
    scratch = [
        *[vm(t.shape, f32) for t in tables],
        vm((n_comp, x_rows, n_y), bf16), vm((n_comp, x_rows, n_y), bf16),
        vm(blocks, f32), vm(blocks, f32), vm(blocks, f32),
        vm((n_y, half), bf16), vm((n_y, half), bf16),
        vm((2, 2, devices * SUB, n_y), bf16), vm((2 * x_rows, devices * SUB), bf16),
        vm((n_k, SUB, width + LANE), f32), vm((n_k, SUB, width + LANE), f32),
        vm((n_k, SUB, width), f32), vm((n_k, SUB, width), f32),
        vm((2 * m_rows, half), bf16), vm((2 * m_rows, half), bf16),
        vm((2, m_rows, half), f32),
        vm((2 * m_rows, n_y), bf16), vm((2 * m_rows, n_y), bf16),
        vm((SUB, width), f32),
        sem((n_comp, 2)), sem((5,)), sem, sem, sem, sem,
        *[sem((n_chunk, 2))] * 3, sem((n_chunk, n_comp, 2)),
    ]
    dims = (n_layer, n_row, n_comp, x_rows, n_y, kept, n_chunk)
    anywhere = pl.BlockSpec(memory_space=pl.ANY)
    return pl.pallas_call(
        functools.partial(fused_kernel, dims),
        out_shape=pltpu.VMEM((n_comp, x_rows, n_y), f32),
        in_specs=[anywhere] * 6,
        out_specs=pl.BlockSpec(memory_space=pltpu.VMEM),
        scratch_shapes=scratch,
        compiler_params=pltpu.CompilerParams(
            collective_id=0, has_side_effects=True, vmem_limit_bytes=54 * 2**20
        ),
    )(magnet, kernel.reshape(n_k, block, n_x), *[jnp.asarray(t) for t in tables]).reshape(magnet.shape)


def fits(magnet, kernel):
    n_layer = lax.axis_size("layer")
    n_row = lax.axis_size("row")
    x_rows, n_y = magnet.shape[2:]
    block, n_x = kernel.shape[2:]
    return (
        n_x == n_y and n_x // 2 % 512 == 0 and x_rows % 256 == 0 and n_row % 2 == 0
        and n_layer % 2 == 0 and block % 32 == 0 and x_rows * n_row == n_x and kernel.shape[0] == 2 * n_layer - 1
    )


def local(magnet, kernel):
    if fits(magnet, kernel):
        return fused(magnet, kernel)
    return general(magnet, kernel)


def solution(mesh):
    in_specs = (P(None, "layer", "row", None), P(None, None, ("layer", "row"), None))
    out_specs = P(None, "layer", "row", None)
    return jax.shard_map(local, mesh=mesh, in_specs=in_specs, out_specs=out_specs, check_vma=False)
```
